32 devices in a mesh: dm: 4 (over z), tm: 8 (over y, x, core).
Axes of the slice: x: 2, y: 2, z: 4, core: 2. Of those that a mesh axis runs over, the one named last changes fastest.
Arguments:
- dispersed: float32 [1024, 8192], P('dm', 'tm')
- widths: int32 [4], replicated, may hold values from 1 to 129, as said below
Outputs:
- snr: bfloat16 [4, 1024, 8192], P(None, 'dm', 'tm')
- peaks: float32 [4, 1024], P(None, 'dm')
The draws below stay inside these ranges and needn't reach their ends.
Inputs may be any that keep to these rules, and one draw needn't show every extreme that they name: `widths`: at least one width equals 129.
All inputs are finite; a program needn't handle non-finite values.
Results may differ from the reference program's by a relative error of at most 0.001.
Values sent between devices are 32-bit elements; how exact they have to be, the bound alone decides.
A program may use at most 64 MiB of HBM per device.

```python
import math
import jax
import jax.numpy as jnp
from jax import lax

DM_DEV = 256
HALF = 128
WMAX = 129
NBOX = 4
TRIAL_MEASURES = 1024
TIME_SAMPLES = 8192


def draw_dispersed(key, part):
    random_key_list = jax.random.split(key, 8)
    trial_row_axis = jnp.arange(TRIAL_MEASURES, dtype=jnp.float32)[:, None]
    time_axis = jnp.arange(TIME_SAMPLES, dtype=jnp.float32)[None, :]
    row_spread_scale = jnp.exp(jax.random.uniform(random_key_list[0], (TRIAL_MEASURES, 1), jnp.float32) * math.log(10.0))
    sample_time_scale = jnp.exp(math.log(3.0) * time_axis / TIME_SAMPLES)
    random_perturbation = jax.random.normal(random_key_list[1], (TRIAL_MEASURES, TIME_SAMPLES), jnp.float32)
    offset_scale = 3.0
    pulse_level = 8.0
    offsets = jax.random.normal(random_key_list[2], (TRIAL_MEASURES, 1), jnp.float32) * offset_scale
    amplitude = jax.random.uniform(random_key_list[3], (TRIAL_MEASURES, 1), jnp.float32) * 5.0
    cycles = 1.0 + 3.0 * jax.random.uniform(random_key_list[4], (TRIAL_MEASURES, 1), jnp.float32)
    phase_shift = jax.random.uniform(random_key_list[5], (TRIAL_MEASURES, 1), jnp.float32) * 2.0 * math.pi
    slope_component = offsets + amplitude * jnp.sin(2.0 * math.pi * cycles * time_axis / TIME_SAMPLES + phase_shift)
    pulse_events = jnp.where(jax.random.uniform(random_key_list[6], (TIME_SAMPLES,), jnp.float32) < 0.02, jax.random.normal(random_key_list[7], (TIME_SAMPLES,), jnp.float32) * pulse_level, 0.0)
    pulse_gain = 1.0 + 2.0 * trial_row_axis / TRIAL_MEASURES
    return row_spread_scale * sample_time_scale * random_perturbation + slope_component + pulse_gain * pulse_events[None, :]


def draw_widths(key, part):
    random_key_list = jax.random.split(key, 2)
    width_draw = jax.random.randint(random_key_list[0], (NBOX,), 1, WMAX + 1, jnp.int32)
    chosen = jax.random.randint(random_key_list[1], (), 0, NBOX, jnp.int32)
    return jnp.where(jnp.arange(NBOX, dtype=jnp.int32) == chosen, WMAX, width_draw).astype(jnp.int32)


def setup_inputs(seed: int = 0) -> dict:
    arg_keys = jax.random.split(jax.random.key(seed), 3)
    return {
        "dispersed": draw_dispersed(jax.random.fold_in(arg_keys[2], 71), 0),
        "widths": draw_widths(jax.random.fold_in(arg_keys[2], 71), 0),
    }


eps_value = 1e-06

def band_table(span_list, block_len):
    column_idx = jnp.arange(span_list.shape[0] * block_len, dtype=jnp.int32)
    offsets = column_idx % block_len
    reaches = jnp.repeat(span_list, block_len)
    row_idx = jnp.arange(2 * block_len, dtype=jnp.int32)[:, None]
    inside = (row_idx >= offsets[None, :]) & (row_idx < offsets[None, :] + reaches[None, :])
    return inside.astype(jnp.float32)

def window_sum(extended, length, band_matrix, block_len):
    row_count = extended.shape[0]
    block_count = length // block_len
    blocks = extended[:, :length + block_len].reshape(row_count, block_count + 1, block_len)
    paired = jnp.concatenate([blocks[:, :-1], blocks[:, 1:]], axis=2)
    return jnp.einsum('rbs,sk->rbk', paired, band_matrix, precision=lax.Precision.HIGHEST)

def boxcar(extended, length, band_matrix, inverse, block_len):
    row_count = extended.shape[0]
    moving = window_sum(extended, length, band_matrix, block_len)
    moving = moving.reshape(row_count, length // block_len, inverse.shape[0], block_len)
    moving = jnp.transpose(moving, (2, 0, 1, 3)).reshape(inverse.shape[0], row_count, length)
    return moving * inverse[:, None, None]

def reference(dispersed, widths):
    row_total, total_len = dispersed.shape
    block_len = 2 * HALF
    ma_band = band_table(jnp.full((1,), 2 * HALF + 1, jnp.int32), block_len)
    box_band = band_table(widths, block_len)
    inverse = 1.0 / jnp.sqrt(widths.astype(jnp.float32))
    positions = jnp.arange(total_len, dtype=jnp.int32)
    counts = (jnp.minimum(positions + HALF, total_len - 1) - jnp.maximum(positions - HALF, 0) + 1).astype(jnp.float32)

    def detrend(row_block):
        row_count = row_block.shape[0]
        first_mean = window_sum(jnp.pad(row_block, ((0, 0), (HALF, HALF))), total_len, ma_band, block_len).reshape(row_count, total_len) / counts
        smooth_mean = window_sum(jnp.pad(first_mean, ((0, 0), (HALF, HALF))), total_len, ma_band, block_len).reshape(row_count, total_len) / counts
        return row_block - smooth_mean
    grouped = dispersed.reshape(row_total // DM_DEV, DM_DEV, total_len)
    detrended = lax.map(detrend, grouped).reshape(row_total, total_len)
    power_sum = lax.optimization_barrier(jnp.sum(detrended * detrended, axis=1))
    row_spread_scale = jnp.sqrt(power_sum / total_len + eps_value)
    normed = detrended / row_spread_scale[:, None]
    common = lax.optimization_barrier(jnp.sum(normed, axis=0)) / row_total
    cleaned = normed - common[None, :]

    def filtered(row_block):
        series = boxcar(jnp.pad(row_block, ((0, 0), (0, block_len))), total_len, box_band, inverse, block_len)
        return (series.astype(jnp.bfloat16), lax.optimization_barrier(jnp.max(series, axis=2)))
    series, peak_values = lax.map(filtered, cleaned.reshape(row_total // DM_DEV, DM_DEV, total_len))
    snr = jnp.transpose(series, (1, 0, 2, 3)).reshape(NBOX, row_total, total_len)
    peaks = jnp.transpose(peak_values, (1, 0, 2)).reshape(NBOX, row_total)
    return (snr, peaks)
```

```python
import functools

import jax
import jax.numpy as jnp
from jax import lax
from jax.experimental import pallas as pl
from jax.experimental.pallas import tpu as pltpu
from jax.sharding import PartitionSpec as P

HALF = 128
BLK = 2 * HALF
LANES = 128
ROWS_STEP = 64
PIECES = 3
EPS = 1e-06
MESH = pl.DeviceIdType.MESH
F32 = jnp.float32
BF16 = jnp.bfloat16


def pieces_of(value):
    out = []
    for _ in range(PIECES):
        term = value.astype(BF16)
        out.append(term)
        value = value - term.astype(F32)
    return out


def put_pieces(ref, start, value):
    for p, term in enumerate(pieces_of(value)):
        ref[p, :, start : start + value.shape[1]] = term


def window_dot(ref, start, reach, band):
    total = None
    for p in range(PIECES):
        part = jnp.dot(ref[p, :, start : start + reach], band, preferred_element_type=F32)
        total = part if total is None else total + part
    return total


def kernel(
    n_tm, n_dm, widths_ref, x_ref, snr_ref, peaks_ref,
    xe, xs, fms, det, ds, boxes, band, box_band, power, colsum, top, best,
    load_sem, halo_send, halo_recv, power_send, power_recv, col_send, col_recv, top_send, top_recv,
):
    rows, length = x_ref.shape
    nbox = widths_ref.shape[0]
    blocks = length // BLK
    total_len = n_tm * length
    me = lax.axis_index("tm")
    mine = lax.axis_index("dm")
    offset = me * length
    has_left, has_right = me > 0, me < n_tm - 1
    edge = BLK + length

    def load(k, start, size):
        return pltpu.make_async_copy(
            x_ref.at[:, pl.ds(start, size)], xe.at[:, pl.ds(BLK + start, size)], load_sem.at[k]
        )

    loads = [load(0, 0, BLK), load(1, length - BLK, BLK), load(2, BLK, length - 2 * BLK)]
    for one in loads:
        one.start()

    barrier = pltpu.get_barrier_semaphore()
    for d in range(1, n_tm):
        pl.semaphore_signal(barrier, inc=1, device_id={"tm": lax.rem(me + d, n_tm)}, device_id_type=MESH)
    for d in range(1, n_dm):
        pl.semaphore_signal(barrier, inc=1, device_id={"dm": lax.rem(mine + d, n_dm)}, device_id_type=MESH)

    rows_i = lax.broadcasted_iota(jnp.int32, (2 * BLK, BLK), 0)
    cols_i = lax.broadcasted_iota(jnp.int32, (2 * BLK, BLK), 1)
    band[...] = jnp.where((rows_i >= cols_i) & (rows_i <= cols_i + BLK), 1.0, 0.0).astype(BF16)
    rows_b = lax.broadcasted_iota(jnp.int32, (BLK + HALF, BLK), 0)
    cols_b = lax.broadcasted_iota(jnp.int32, (BLK + HALF, BLK), 1)
    lag = rows_b - cols_b
    for i in range(nbox):
        hit = (lag >= 0) & (lag < widths_ref[i])
        box_band[:, i * BLK : (i + 1) * BLK] = jnp.where(hit, 1.0, 0.0).astype(BF16)

    pl.semaphore_wait(barrier, n_tm - 1 + n_dm - 1)

    right = {"tm": lax.rem(me + 1, n_tm)}
    left = {"tm": lax.rem(me + n_tm - 1, n_tm)}

    def move(src, dst, k, target):
        return pltpu.make_async_remote_copy(
            src_ref=src, dst_ref=dst, send_sem=halo_send.at[k], recv_sem=halo_recv.at[k],
            device_id=target, device_id_type=MESH,
        )

    to_right = move(xe.at[:, pl.ds(length, BLK)], xe.at[:, pl.ds(0, BLK)], 0, right)
    to_left = move(xe.at[:, pl.ds(BLK, BLK)], xe.at[:, pl.ds(edge, BLK)], 1, left)
    head = move(det.at[:, pl.ds(0, HALF)], det.at[:, pl.ds(length, HALF)], 2, left)

    loads[1].wait()

    @pl.when(has_right)
    def _():
        to_right.start()

    loads[0].wait()

    @pl.when(has_left)
    def _():
        to_left.start()

    @pl.when(jnp.logical_not(has_left))
    def _():
        xe[:, 0:BLK] = jnp.zeros((rows, BLK), F32)

    @pl.when(jnp.logical_not(has_right))
    def _():
        xe[:, edge : edge + BLK] = jnp.zeros((rows, BLK), F32)
        det[:, length : length + HALF] = jnp.zeros((rows, HALF), F32)

    loads[2].wait()

    def inverse_counts(first):
        pos = offset + first + lax.broadcasted_iota(jnp.int32, (1, BLK), 1)
        counts = jnp.minimum(pos + HALF, total_len - 1) - jnp.maximum(pos - HALF, 0) + 1
        inside = (pos >= 0) & (pos < total_len)
        return jnp.where(inside, 1.0 / counts.astype(F32), 0.0)

    def first_mean(j):
        sums = window_dot(xs, j * BLK, 2 * BLK, band[...])
        put_pieces(fms, j * BLK, sums * inverse_counts(j * BLK - HALF))

    def detrend(j):
        sums = window_dot(fms, j * BLK, 2 * BLK, band[...])
        value = xe[:, (j + 1) * BLK : (j + 2) * BLK] - sums * inverse_counts(j * BLK)
        det[:, j * BLK : (j + 1) * BLK] = value
        put_pieces(ds, j * BLK, value)

    for j in range(1, blocks + 1):
        put_pieces(xs, j * BLK, xe[:, j * BLK : (j + 1) * BLK])
    for j in range(1, blocks):
        first_mean(j)
    for j in range(1, blocks - 1):
        detrend(j)

    @pl.when(has_left)
    def _():
        to_right.wait_recv()

    put_pieces(xs, 0, xe[:, 0:BLK])
    first_mean(0)
    detrend(0)

    @pl.when(has_left)
    def _():
        head.start()

    @pl.when(has_right)
    def _():
        to_left.wait_recv()

    put_pieces(xs, edge, xe[:, edge : edge + BLK])
    first_mean(blocks)
    detrend(blocks - 1)

    def exchange(slots, send, recv, axis, size, index):
        copies = []
        for d in range(1, size):
            copies.append(
                pltpu.make_async_remote_copy(
                    src_ref=slots.at[0], dst_ref=slots.at[d], send_sem=send.at[d], recv_sem=recv.at[d],
                    device_id={axis: lax.rem(index + d, size)}, device_id_type=MESH,
                )
            )
        for one in copies:
            one.start()
        return copies

    squares = jnp.zeros((rows, LANES), F32)
    for c in range(length // LANES):
        part = det[:, c * LANES : (c + 1) * LANES]
        squares = squares + part * part
    power[0] = jnp.sum(jnp.transpose(squares), axis=0, keepdims=True)
    power_copies = exchange(power, power_send, power_recv, "tm", n_tm, me)

    def boxcar(j):
        sums = window_dot(ds, j * BLK, BLK + HALF, box_band[...])
        for i in range(nbox):
            boxes[i, :, j * BLK : (j + 1) * BLK] = sums[:, i * BLK : (i + 1) * BLK]

    early = blocks // 2
    for j in range(early):
        boxcar(j)

    @pl.when(has_right)
    def _():
        head.wait_recv()

    put_pieces(ds, length, det[:, length : length + HALF])

    for one in power_copies:
        one.wait_recv()
    power_sum = power[0]
    for d in range(1, n_tm):
        power_sum = power_sum + power[d]
    scale = 1.0 / jnp.sqrt(power_sum / total_len + EPS)
    scale_rows = jnp.transpose(jnp.broadcast_to(scale, (LANES, rows)))
    for c in range(length // LANES + 1):
        part = det[:, c * LANES : (c + 1) * LANES] * scale_rows
        colsum[0, :, c * LANES : (c + 1) * LANES] = jnp.sum(part, axis=0, keepdims=True)
    col_copies = exchange(colsum, col_send, col_recv, "dm", n_dm, mine)

    for j in range(early, blocks):
        boxcar(j)

    for one in col_copies:
        one.wait_recv()
    common = colsum[0]
    for d in range(1, n_dm):
        common = common + colsum[d]
    common = common / (rows * n_dm)
    lines = [common[:, j * BLK : (j + 1) * BLK + HALF] for j in range(blocks)]
    lines = lines + [jnp.zeros((-blocks % 8, BLK + HALF), F32)] if blocks % 8 else lines
    stacked = jnp.concatenate(lines, axis=0)
    common_boxes = None
    for term in pieces_of(stacked):
        part = jnp.dot(term, box_band[...], preferred_element_type=F32)
        common_boxes = part if common_boxes is None else common_boxes + part

    for i in range(nbox):
        width = jnp.full((1, LANES), widths_ref[i], jnp.int32).astype(F32)
        inverse = 1.0 / jnp.sqrt(width)
        rows_of = []
        for c in range(length // LANES):
            j, part = divmod(c * LANES, BLK)
            first = i * BLK + part
            rows_of.append(common_boxes[j : j + 1, first : first + LANES] * inverse)
        best_tops = []
        for r in range(rows // ROWS_STEP):
            span = slice(r * ROWS_STEP, (r + 1) * ROWS_STEP)
            factor = scale_rows[span] * inverse
            peak = None
            for c in range(length // LANES):
                cols = slice(c * LANES, (c + 1) * LANES)
                series = boxes[i, span, cols] * factor - rows_of[c]
                snr_ref[i, span, cols] = series.astype(BF16)
                peak = series if peak is None else jnp.maximum(peak, series)
            best[span, :] = peak
        top[0, i : i + 1, :] = jnp.max(jnp.transpose(best[...]), axis=0, keepdims=True)

    top_copies = exchange(top, top_send, top_recv, "tm", n_tm, me)
    for one in top_copies:
        one.wait_recv()
    peaks = top[0]
    for d in range(1, n_tm):
        peaks = jnp.maximum(peaks, top[d])
    peaks_ref[...] = peaks

    for one in power_copies + col_copies + top_copies:
        one.wait_send()

    @pl.when(has_right)
    def _():
        to_right.wait_send()

    @pl.when(has_left)
    def _():
        to_left.wait_send()
        head.wait_send()


def body(n_tm, n_dm, dispersed, widths):
    rows, length = dispersed.shape
    nbox = widths.shape[0]
    sems = pltpu.SemaphoreType.DMA
    return pl.pallas_call(
        functools.partial(kernel, n_tm, n_dm),
        out_shape=(
            jax.ShapeDtypeStruct((nbox, rows, length), BF16),
            jax.ShapeDtypeStruct((nbox, rows), F32),
        ),
        in_specs=[pl.BlockSpec(memory_space=pltpu.SMEM), pl.BlockSpec(memory_space=pl.ANY)],
        out_specs=(pl.BlockSpec(memory_space=pltpu.VMEM), pl.BlockSpec(memory_space=pltpu.VMEM)),
        scratch_shapes=[
            pltpu.VMEM((rows, length + 2 * BLK), F32),
            pltpu.VMEM((PIECES, rows, length + 2 * BLK), BF16),
            pltpu.VMEM((PIECES, rows, length + BLK), BF16),
            pltpu.VMEM((rows, length + HALF), F32),
            pltpu.VMEM((PIECES, rows, length + HALF), BF16),
            pltpu.VMEM((nbox, rows, length), F32),
            pltpu.VMEM((2 * BLK, BLK), BF16),
            pltpu.VMEM((BLK + HALF, nbox * BLK), BF16),
            pltpu.VMEM((n_tm, 1, rows), F32),
            pltpu.VMEM((n_dm, 1, length + HALF), F32),
            pltpu.VMEM((n_tm, nbox, rows), F32),
            pltpu.VMEM((rows, LANES), F32),
            sems((3,)), sems((3,)), sems((3,)),
            sems((n_tm,)), sems((n_tm,)),
            sems((n_dm,)), sems((n_dm,)),
            sems((n_tm,)), sems((n_tm,)),
        ],
        compiler_params=pltpu.CompilerParams(
            collective_id=0, has_side_effects=True, vmem_limit_bytes=40 * 1024 * 1024
        ),
        name="detrend_filter",
    )(widths, dispersed)


def solution(mesh):
    return jax.shard_map(
        functools.partial(body, mesh.shape["tm"], mesh.shape["dm"]),
        mesh=mesh,
        in_specs=(P("dm", "tm"), P()),
        out_specs=(P(None, "dm", "tm"), P(None, "dm")),
        check_vma=False,
    )
```

```python
import functools

import jax
import jax.numpy as jnp
from jax import lax
from jax.experimental import pallas as pl
from jax.experimental.pallas import tpu as pltpu
from jax.sharding import PartitionSpec as P

HALF = 128
BLK = 2 * HALF
LANES = 128
ROWS_STEP = 64
PIECES = 3
EPS = 1e-06
MESH = pl.DeviceIdType.MESH
F32 = jnp.float32
BF16 = jnp.bfloat16


def pieces_of(value):
    out = []
    for _ in range(PIECES):
        term = value.astype(BF16)
        out.append(term)
        value = value - term.astype(F32)
    return out


def put_pieces(ref, start, value):
    for p, term in enumerate(pieces_of(value)):
        ref[p, :, start : start + value.shape[1]] = term


def window_dot(ref, start, reach, band):
    total = None
    for p in range(PIECES):
        part = jnp.dot(ref[p, :, start : start + reach], band, preferred_element_type=F32)
        total = part if total is None else total + part
    return total


def kernel(
    n_tm, n_dm, widths_hbm, x_ref, snr_ref, peaks_ref,
    widths_ref, xe, xs, fms, det, ds, boxes, band, box_band, power, colsum, top, best,
    width_sem, load_sem, halo_send, halo_recv, power_send, power_recv, col_send, col_recv, top_send, top_recv,
):
    rows, length = x_ref.shape
    nbox = widths_hbm.shape[0]
    blocks = length // BLK
    total_len = n_tm * length
    me = lax.axis_index("tm")
    mine = lax.axis_index("dm")
    offset = me * length
    has_left, has_right = me > 0, me < n_tm - 1
    edge = BLK + length

    def load(k, start, size):
        return pltpu.make_async_copy(
            x_ref.at[:, pl.ds(start, size)], xe.at[:, pl.ds(BLK + start, size)], load_sem.at[k]
        )

    loads = [load(0, 0, BLK), load(1, length - BLK, BLK), load(2, BLK, length - 2 * BLK)]
    width_load = pltpu.make_async_copy(widths_hbm, widths_ref, width_sem)
    width_load.start()
    for one in loads:
        one.start()

    barrier = pltpu.get_barrier_semaphore()
    for d in range(1, n_tm):
        pl.semaphore_signal(barrier, inc=1, device_id={"tm": lax.rem(me + d, n_tm)}, device_id_type=MESH)
    for d in range(1, n_dm):
        pl.semaphore_signal(barrier, inc=1, device_id={"dm": lax.rem(mine + d, n_dm)}, device_id_type=MESH)

    rows_i = lax.broadcasted_iota(jnp.int32, (2 * BLK, BLK), 0)
    cols_i = lax.broadcasted_iota(jnp.int32, (2 * BLK, BLK), 1)
    band[...] = jnp.where((rows_i >= cols_i) & (rows_i <= cols_i + BLK), 1.0, 0.0).astype(BF16)
    width_load.wait()
    rows_b = lax.broadcasted_iota(jnp.int32, (BLK + HALF, BLK), 0)
    cols_b = lax.broadcasted_iota(jnp.int32, (BLK + HALF, BLK), 1)
    lag = rows_b - cols_b
    for i in range(nbox):
        hit = (lag >= 0) & (lag < widths_ref[i])
        box_band[:, i * BLK : (i + 1) * BLK] = jnp.where(hit, 1.0, 0.0).astype(BF16)

    pl.semaphore_wait(barrier, n_tm - 1 + n_dm - 1)

    right = {"tm": lax.rem(me + 1, n_tm)}
    left = {"tm": lax.rem(me + n_tm - 1, n_tm)}

    def move(src, dst, k, target):
        return pltpu.make_async_remote_copy(
            src_ref=src, dst_ref=dst, send_sem=halo_send.at[k], recv_sem=halo_recv.at[k],
            device_id=target, device_id_type=MESH,
        )

    to_right = move(xe.at[:, pl.ds(length, BLK)], xe.at[:, pl.ds(0, BLK)], 0, right)
    to_left = move(xe.at[:, pl.ds(BLK, BLK)], xe.at[:, pl.ds(edge, BLK)], 1, left)
    head = move(det.at[:, pl.ds(0, HALF)], det.at[:, pl.ds(length, HALF)], 2, left)

    loads[1].wait()

    @pl.when(has_right)
    def _():
        to_right.start()

    loads[0].wait()

    @pl.when(has_left)
    def _():
        to_left.start()

    @pl.when(jnp.logical_not(has_left))
    def _():
        xe[:, 0:BLK] = jnp.zeros((rows, BLK), F32)

    @pl.when(jnp.logical_not(has_right))
    def _():
        xe[:, edge : edge + BLK] = jnp.zeros((rows, BLK), F32)
        det[:, length : length + HALF] = jnp.zeros((rows, HALF), F32)

    loads[2].wait()

    def inverse_counts(first):
        pos = offset + first + lax.broadcasted_iota(jnp.int32, (1, BLK), 1)
        counts = jnp.minimum(pos + HALF, total_len - 1) - jnp.maximum(pos - HALF, 0) + 1
        inside = (pos >= 0) & (pos < total_len)
        return jnp.where(inside, 1.0 / counts.astype(F32), 0.0)

    def first_mean(j):
        sums = window_dot(xs, j * BLK, 2 * BLK, band[...])
        put_pieces(fms, j * BLK, sums * inverse_counts(j * BLK - HALF))

    def detrend(j):
        sums = window_dot(fms, j * BLK, 2 * BLK, band[...])
        value = xe[:, (j + 1) * BLK : (j + 2) * BLK] - sums * inverse_counts(j * BLK)
        det[:, j * BLK : (j + 1) * BLK] = value
        put_pieces(ds, j * BLK, value)

    for j in range(1, blocks + 1):
        put_pieces(xs, j * BLK, xe[:, j * BLK : (j + 1) * BLK])
    for j in range(1, blocks):
        first_mean(j)
    for j in range(1, blocks - 1):
        detrend(j)

    @pl.when(has_left)
    def _():
        to_right.wait_recv()

    put_pieces(xs, 0, xe[:, 0:BLK])
    first_mean(0)
    detrend(0)

    @pl.when(has_left)
    def _():
        head.start()

    @pl.when(has_right)
    def _():
        to_left.wait_recv()

    put_pieces(xs, edge, xe[:, edge : edge + BLK])
    first_mean(blocks)
    detrend(blocks - 1)

    def exchange(slots, send, recv, axis, size, index):
        copies = []
        for d in range(1, size):
            copies.append(
                pltpu.make_async_remote_copy(
                    src_ref=slots.at[0], dst_ref=slots.at[d], send_sem=send.at[d], recv_sem=recv.at[d],
                    device_id={axis: lax.rem(index + d, size)}, device_id_type=MESH,
                )
            )
        for one in copies:
            one.start()
        return copies

    squares = jnp.zeros((rows, LANES), F32)
    for c in range(length // LANES):
        part = det[:, c * LANES : (c + 1) * LANES]
        squares = squares + part * part
    power[0] = jnp.sum(jnp.transpose(squares), axis=0, keepdims=True)
    power_copies = exchange(power, power_send, power_recv, "tm", n_tm, me)

    def boxcar(j):
        sums = window_dot(ds, j * BLK, BLK + HALF, box_band[...])
        for i in range(nbox):
            boxes[i, :, j * BLK : (j + 1) * BLK] = sums[:, i * BLK : (i + 1) * BLK]

    early = blocks // 2
    for j in range(early):
        boxcar(j)

    @pl.when(has_right)
    def _():
        head.wait_recv()

    put_pieces(ds, length, det[:, length : length + HALF])

    for one in power_copies:
        one.wait_recv()
    power_sum = power[0]
    for d in range(1, n_tm):
        power_sum = power_sum + power[d]
    scale = 1.0 / jnp.sqrt(power_sum / total_len + EPS)
    scale_rows = jnp.transpose(jnp.broadcast_to(scale, (LANES, rows)))
    for c in range(length // LANES + 1):
        part = det[:, c * LANES : (c + 1) * LANES] * scale_rows
        colsum[0, :, c * LANES : (c + 1) * LANES] = jnp.sum(part, axis=0, keepdims=True)
    col_copies = exchange(colsum, col_send, col_recv, "dm", n_dm, mine)

    for j in range(early, blocks):
        boxcar(j)

    for one in col_copies:
        one.wait_recv()
    common = colsum[0]
    for d in range(1, n_dm):
        common = common + colsum[d]
    common = common / (rows * n_dm)
    lines = [common[:, j * BLK : (j + 1) * BLK + HALF] for j in range(blocks)]
    lines = lines + [jnp.zeros((-blocks % 8, BLK + HALF), F32)] if blocks % 8 else lines
    stacked = jnp.concatenate(lines, axis=0)
    common_boxes = None
    for term in pieces_of(stacked):
        part = jnp.dot(term, box_band[...], preferred_element_type=F32)
        common_boxes = part if common_boxes is None else common_boxes + part

    def each_series(use):
        for i in range(nbox):
            width = jnp.full((1, LANES), widths_ref[i], jnp.int32).astype(F32)
            inverse = 1.0 / jnp.sqrt(width)
            shifts = []
            for c in range(length // LANES):
                j, part = divmod(c * LANES, BLK)
                first = i * BLK + part
                shifts.append(common_boxes[j : j + 1, first : first + LANES] * inverse)
            for r in range(rows // ROWS_STEP):
                span = slice(r * ROWS_STEP, (r + 1) * ROWS_STEP)
                factor = scale_rows[span] * inverse
                use(i, span, [
                    boxes[i, span, c * LANES : (c + 1) * LANES] * factor - shifts[c]
                    for c in range(length // LANES)
                ])

    def take_peak(i, span, parts):
        best[i, span, :] = functools.reduce(jnp.maximum, parts)

    def take_snr(i, span, parts):
        for c, series in enumerate(parts):
            snr_ref[i, span, c * LANES : (c + 1) * LANES] = series.astype(BF16)

    each_series(take_peak)
    for i in range(nbox):
        top[0, i : i + 1, :] = jnp.max(jnp.transpose(best[i]), axis=0, keepdims=True)

    top_copies = exchange(top, top_send, top_recv, "tm", n_tm, me)
    each_series(take_snr)
    for one in top_copies:
        one.wait_recv()
    peaks = top[0]
    for d in range(1, n_tm):
        peaks = jnp.maximum(peaks, top[d])
    peaks_ref[...] = peaks

    for one in power_copies + col_copies + top_copies:
        one.wait_send()

    @pl.when(has_right)
    def _():
        to_right.wait_send()

    @pl.when(has_left)
    def _():
        to_left.wait_send()
        head.wait_send()


def hand_out(snr_ref, peaks_ref, snr_out, peaks_out, sem):
    nbox = snr_ref.shape[0]
    copies = [pltpu.make_async_copy(snr_ref.at[i], snr_out.at[i], sem.at[i]) for i in range(nbox)]
    copies.append(pltpu.make_async_copy(peaks_ref, peaks_out, sem.at[nbox]))
    for one in copies:
        one.start()
    for one in copies:
        one.wait()


def body(n_tm, n_dm, dispersed, widths):
    rows, length = dispersed.shape
    nbox = widths.shape[0]
    sems = pltpu.SemaphoreType.DMA
    snr, peaks = pl.pallas_call(
        functools.partial(kernel, n_tm, n_dm),
        out_shape=(
            jax.ShapeDtypeStruct((nbox, rows, length), BF16),
            jax.ShapeDtypeStruct((nbox, rows), F32),
        ),
        in_specs=[pl.BlockSpec(memory_space=pltpu.HBM)] * 2,
        out_specs=(pl.BlockSpec(memory_space=pltpu.VMEM), pl.BlockSpec(memory_space=pltpu.VMEM)),
        scratch_shapes=[
            pltpu.SMEM((nbox,), jnp.int32),
            pltpu.VMEM((rows, length + 2 * BLK), F32),
            pltpu.VMEM((PIECES, rows, length + 2 * BLK), BF16),
            pltpu.VMEM((PIECES, rows, length + BLK), BF16),
            pltpu.VMEM((rows, length + HALF), F32),
            pltpu.VMEM((PIECES, rows, length + HALF), BF16),
            pltpu.VMEM((nbox, rows, length), F32),
            pltpu.VMEM((2 * BLK, BLK), BF16),
            pltpu.VMEM((BLK + HALF, nbox * BLK), BF16),
            pltpu.VMEM((n_tm, 1, rows), F32),
            pltpu.VMEM((n_dm, 1, length + HALF), F32),
            pltpu.VMEM((n_tm, nbox, rows), F32),
            pltpu.VMEM((nbox, rows, LANES), F32),
            sems, sems((3,)), sems((3,)), sems((3,)),
            sems((n_tm,)), sems((n_tm,)),
            sems((n_dm,)), sems((n_dm,)),
            sems((n_tm,)), sems((n_tm,)),
        ],
        compiler_params=pltpu.CompilerParams(
            collective_id=0, has_side_effects=True, vmem_limit_bytes=40 * 1024 * 1024
        ),
        name="detrend_filter",
    )(
        pltpu.with_memory_space_constraint(widths, pltpu.HBM),
        pltpu.with_memory_space_constraint(dispersed, pltpu.HBM),
    )
    return pl.pallas_call(
        hand_out,
        out_shape=(
            jax.ShapeDtypeStruct(snr.shape, BF16),
            jax.ShapeDtypeStruct(peaks.shape, F32),
        ),
        in_specs=[pl.BlockSpec(memory_space=pltpu.VMEM)] * 2,
        out_specs=(pl.BlockSpec(memory_space=pltpu.HBM), pl.BlockSpec(memory_space=pltpu.HBM)),
        scratch_shapes=[sems((nbox + 1,))],
        compiler_params=pltpu.CompilerParams(vmem_limit_bytes=1024 * 1024),
        name="hand_out",
    )(snr, peaks)


def solution(mesh):
    return jax.shard_map(
        functools.partial(body, mesh.shape["tm"], mesh.shape["dm"]),
        mesh=mesh,
        in_specs=(P("dm", "tm"), P()),
        out_specs=(P(None, "dm", "tm"), P(None, "dm")),
        check_vma=False,
    )
```

```python
import functools

import jax
import jax.numpy as jnp
from jax import lax
from jax.experimental import pallas as pl
from jax.experimental.pallas import tpu as pltpu
from jax.sharding import PartitionSpec as P

HALF = 128
BLK = 2 * HALF
LANES = 128
ROWS_STEP = 64
PIECES = 3
EPS = 1e-06
MESH = pl.DeviceIdType.MESH
F32 = jnp.float32
BF16 = jnp.bfloat16


def pieces_of(value):
    out = []
    for _ in range(PIECES):
        term = value.astype(BF16)
        out.append(term)
        value = value - term.astype(F32)
    return out


def put_pieces(ref, start, value):
    for p, term in enumerate(pieces_of(value)):
        ref[p, :, start : start + value.shape[1]] = term


def window_dot(ref, start, reach, band):
    total = None
    for p in range(PIECES):
        part = jnp.dot(ref[p, :, start : start + reach], band, preferred_element_type=F32)
        total = part if total is None else total + part
    return total


def kernel(
    n_tm, n_dm, widths_hbm, x_ref, snr_ref, peaks_ref,
    widths_ref, ahead, squares, xe, xs, fms, det, ds, boxes, band, box_band, power, colsum, top, best,
    width_sem, load_sem, halo_send, halo_recv, power_send, power_recv, col_send, col_recv, top_send, top_recv,
):
    rows, length = x_ref.shape
    nbox = widths_hbm.shape[0]
    blocks = length // BLK
    total_len = n_tm * length
    me = lax.axis_index("tm")
    mine = lax.axis_index("dm")
    offset = me * length
    has_left, has_right = me > 0, me < n_tm - 1
    edge = BLK + length

    def load(k, start, size):
        return pltpu.make_async_copy(
            x_ref.at[:, pl.ds(start, size)], xe.at[:, pl.ds(BLK + start, size)], load_sem.at[k]
        )

    loads = [load(0, 0, BLK), load(1, length - BLK, BLK), load(2, BLK, length - 2 * BLK)]
    width_load = pltpu.make_async_copy(widths_hbm, widths_ref, width_sem)
    width_load.start()
    for one in loads:
        one.start()

    barrier = pltpu.get_barrier_semaphore()
    for d in range(1, n_tm):
        pl.semaphore_signal(barrier, inc=1, device_id={"tm": lax.rem(me + d, n_tm)}, device_id_type=MESH)
    for d in range(1, n_dm):
        pl.semaphore_signal(barrier, inc=1, device_id={"dm": lax.rem(mine + d, n_dm)}, device_id_type=MESH)

    rows_i = lax.broadcasted_iota(jnp.int32, (2 * BLK, BLK), 0)
    cols_i = lax.broadcasted_iota(jnp.int32, (2 * BLK, BLK), 1)
    band[...] = jnp.where((rows_i >= cols_i) & (rows_i <= cols_i + BLK), 1.0, 0.0).astype(BF16)
    width_load.wait()
    rows_b = lax.broadcasted_iota(jnp.int32, (BLK + HALF, BLK), 0)
    cols_b = lax.broadcasted_iota(jnp.int32, (BLK + HALF, BLK), 1)
    lag = rows_b - cols_b
    for i in range(nbox):
        hit = (lag >= 0) & (lag < widths_ref[i])
        box_band[:, i * BLK : (i + 1) * BLK] = jnp.where(hit, 1.0, 0.0).astype(BF16)

    pl.semaphore_wait(barrier, n_tm - 1 + n_dm - 1)

    right = {"tm": lax.rem(me + 1, n_tm)}
    left = {"tm": lax.rem(me + n_tm - 1, n_tm)}

    def move(src, dst, k, target):
        return pltpu.make_async_remote_copy(
            src_ref=src, dst_ref=dst, send_sem=halo_send.at[k], recv_sem=halo_recv.at[k],
            device_id=target, device_id_type=MESH,
        )

    to_right = move(xe.at[:, pl.ds(length, BLK)], xe.at[:, pl.ds(0, BLK)], 0, right)
    to_left = move(xe.at[:, pl.ds(BLK, BLK)], xe.at[:, pl.ds(edge, BLK)], 1, left)
    beyond = move(xe.at[:, pl.ds(2 * BLK, HALF)], xe.at[:, pl.ds(edge + BLK, HALF)], 2, left)

    loads[1].wait()

    @pl.when(has_right)
    def _():
        to_right.start()

    loads[0].wait()

    @pl.when(has_left)
    def _():
        to_left.start()

    @pl.when(jnp.logical_not(has_left))
    def _():
        xe[:, 0:BLK] = jnp.zeros((rows, BLK), F32)

    @pl.when(jnp.logical_not(has_right))
    def _():
        xe[:, edge : edge + BLK + HALF] = jnp.zeros((rows, BLK + HALF), F32)

    loads[2].wait()

    @pl.when(has_left)
    def _():
        beyond.start()

    def inverse_counts(first, size):
        pos = offset + first + lax.broadcasted_iota(jnp.int32, (1, size), 1)
        counts = jnp.minimum(pos + HALF, total_len - 1) - jnp.maximum(pos - HALF, 0) + 1
        inside = (pos >= 0) & (pos < total_len)
        return jnp.where(inside, 1.0 / counts.astype(F32), 0.0)

    def put_mean(start, sums):
        put_pieces(fms, start, sums * inverse_counts(start - HALF, sums.shape[1]))

    def put_detrended(start, sums):
        size = sums.shape[1]
        value = xe[:, BLK + start : BLK + start + size] - sums * inverse_counts(start, size)
        det[:, start : start + size] = value
        put_pieces(ds, start, value)

    def square_sum(first, last):
        total = None
        for c in range(first, last, LANES):
            part = det[:, c : c + LANES]
            total = part * part if total is None else total + part * part
        return total

    def full(ref, start):
        return window_dot(ref, start, 2 * BLK, band[...])

    def upper(ref, start):
        return window_dot(ref, start, BLK, band[0:BLK, :])

    def lower(ref, start):
        return window_dot(ref, start, BLK, band[BLK:, :])

    last = length - BLK
    for j in range(1, blocks + 1):
        put_pieces(xs, j * BLK, xe[:, j * BLK : (j + 1) * BLK])
    for j in range(1, blocks):
        put_mean(j * BLK, full(xs, j * BLK))
    for j in range(1, blocks - 1):
        put_detrended(j * BLK, full(fms, j * BLK))
    ahead[0] = lower(xs, BLK)
    ahead[1] = upper(xs, length)
    ahead[2] = lower(fms, BLK)
    ahead[3] = upper(fms, last)
    squares[...] = square_sum(BLK, last)

    @pl.when(has_left)
    def _():
        to_right.wait_recv()

    put_pieces(xs, 0, xe[:, 0:BLK])
    put_mean(0, ahead[0] + upper(xs, 0))
    put_detrended(0, ahead[2] + upper(fms, 0))
    squares[...] += square_sum(0, BLK)

    @pl.when(has_right)
    def _():
        to_left.wait_recv()

    put_pieces(xs, edge, xe[:, edge : edge + BLK])
    put_mean(length, ahead[1] + lower(xs, edge))
    put_detrended(last, ahead[3] + lower(fms, length))

    def exchange(slots, send, recv, axis, size, index):
        copies = []
        for d in range(1, size):
            copies.append(
                pltpu.make_async_remote_copy(
                    src_ref=slots.at[0], dst_ref=slots.at[d], send_sem=send.at[d], recv_sem=recv.at[d],
                    device_id={axis: lax.rem(index + d, size)}, device_id_type=MESH,
                )
            )
        for one in copies:
            one.start()
        return copies

    all_squares = squares[...] + square_sum(last, length)
    power[0] = jnp.sum(jnp.transpose(all_squares), axis=0, keepdims=True)
    power_copies = exchange(power, power_send, power_recv, "tm", n_tm, me)

    def boxcar(j):
        sums = window_dot(ds, j * BLK, BLK + HALF, box_band[...])
        for i in range(nbox):
            boxes[i, :, j * BLK : (j + 1) * BLK] = sums[:, i * BLK : (i + 1) * BLK]

    early = blocks // 2
    for j in range(early):
        boxcar(j)

    @pl.when(has_right)
    def _():
        beyond.wait_recv()

    short = band[0 : BLK + HALF, 0:HALF]
    put_pieces(xs, edge + BLK, xe[:, edge + BLK : edge + BLK + HALF])
    put_mean(edge, window_dot(xs, edge, BLK + HALF, short))
    put_detrended(length, window_dot(fms, length, BLK + HALF, short))

    for one in power_copies:
        one.wait_recv()
    power_sum = power[0]
    for d in range(1, n_tm):
        power_sum = power_sum + power[d]
    scale = 1.0 / jnp.sqrt(power_sum / total_len + EPS)
    scale_rows = jnp.transpose(jnp.broadcast_to(scale, (LANES, rows)))
    for c in range(length // LANES + 1):
        part = det[:, c * LANES : (c + 1) * LANES] * scale_rows
        colsum[0, :, c * LANES : (c + 1) * LANES] = jnp.sum(part, axis=0, keepdims=True)
    col_copies = exchange(colsum, col_send, col_recv, "dm", n_dm, mine)

    for j in range(early, blocks):
        boxcar(j)

    for one in col_copies:
        one.wait_recv()
    common = colsum[0]
    for d in range(1, n_dm):
        common = common + colsum[d]
    common = common / (rows * n_dm)
    lines = [common[:, j * BLK : (j + 1) * BLK + HALF] for j in range(blocks)]
    lines = lines + [jnp.zeros((-blocks % 8, BLK + HALF), F32)] if blocks % 8 else lines
    stacked = jnp.concatenate(lines, axis=0)
    common_boxes = None
    for term in pieces_of(stacked):
        part = jnp.dot(term, box_band[...], preferred_element_type=F32)
        common_boxes = part if common_boxes is None else common_boxes + part

    def each_series(use):
        for i in range(nbox):
            width = jnp.full((1, LANES), widths_ref[i], jnp.int32).astype(F32)
            inverse = 1.0 / jnp.sqrt(width)
            shifts = []
            for c in range(length // LANES):
                j, part = divmod(c * LANES, BLK)
                first = i * BLK + part
                shifts.append(common_boxes[j : j + 1, first : first + LANES] * inverse)
            for r in range(rows // ROWS_STEP):
                span = slice(r * ROWS_STEP, (r + 1) * ROWS_STEP)
                factor = scale_rows[span] * inverse
                use(i, span, [
                    boxes[i, span, c * LANES : (c + 1) * LANES] * factor - shifts[c]
                    for c in range(length // LANES)
                ])

    def take_peak(i, span, parts):
        best[i, span, :] = functools.reduce(jnp.maximum, parts)

    def take_snr(i, span, parts):
        for c, series in enumerate(parts):
            snr_ref[i, span, c * LANES : (c + 1) * LANES] = series.astype(BF16)

    each_series(take_peak)
    for i in range(nbox):
        top[0, i : i + 1, :] = jnp.max(jnp.transpose(best[i]), axis=0, keepdims=True)

    top_copies = exchange(top, top_send, top_recv, "tm", n_tm, me)
    each_series(take_snr)
    for one in top_copies:
        one.wait_recv()
    peaks = top[0]
    for d in range(1, n_tm):
        peaks = jnp.maximum(peaks, top[d])
    peaks_ref[...] = peaks

    for one in power_copies + col_copies + top_copies:
        one.wait_send()

    @pl.when(has_right)
    def _():
        to_right.wait_send()

    @pl.when(has_left)
    def _():
        to_left.wait_send()
        beyond.wait_send()


def hand_out(snr_ref, peaks_ref, snr_out, peaks_out, sem):
    nbox = snr_ref.shape[0]
    copies = [pltpu.make_async_copy(snr_ref.at[i], snr_out.at[i], sem.at[i]) for i in range(nbox)]
    copies.append(pltpu.make_async_copy(peaks_ref, peaks_out, sem.at[nbox]))
    for one in copies:
        one.start()
    for one in copies:
        one.wait()


def body(n_tm, n_dm, dispersed, widths):
    rows, length = dispersed.shape
    nbox = widths.shape[0]
    sems = pltpu.SemaphoreType.DMA
    snr, peaks = pl.pallas_call(
        functools.partial(kernel, n_tm, n_dm),
        out_shape=(
            jax.ShapeDtypeStruct((nbox, rows, length), BF16),
            jax.ShapeDtypeStruct((nbox, rows), F32),
        ),
        in_specs=[pl.BlockSpec(memory_space=pltpu.HBM)] * 2,
        out_specs=(pl.BlockSpec(memory_space=pltpu.VMEM), pl.BlockSpec(memory_space=pltpu.VMEM)),
        scratch_shapes=[
            pltpu.SMEM((nbox,), jnp.int32),
            pltpu.VMEM((4, rows, BLK), F32),
            pltpu.VMEM((rows, LANES), F32),
            pltpu.VMEM((rows, length + 2 * BLK + HALF), F32),
            pltpu.VMEM((PIECES, rows, length + 2 * BLK + HALF), BF16),
            pltpu.VMEM((PIECES, rows, length + BLK + HALF), BF16),
            pltpu.VMEM((rows, length + HALF), F32),
            pltpu.VMEM((PIECES, rows, length + HALF), BF16),
            pltpu.VMEM((nbox, rows, length), F32),
            pltpu.VMEM((2 * BLK, BLK), BF16),
            pltpu.VMEM((BLK + HALF, nbox * BLK), BF16),
            pltpu.VMEM((n_tm, 1, rows), F32),
            pltpu.VMEM((n_dm, 1, length + HALF), F32),
            pltpu.VMEM((n_tm, nbox, rows), F32),
            pltpu.VMEM((nbox, rows, LANES), F32),
            sems, sems((3,)), sems((3,)), sems((3,)),
            sems((n_tm,)), sems((n_tm,)),
            sems((n_dm,)), sems((n_dm,)),
            sems((n_tm,)), sems((n_tm,)),
        ],
        compiler_params=pltpu.CompilerParams(
            collective_id=0, has_side_effects=True, vmem_limit_bytes=40 * 1024 * 1024
        ),
        name="detrend_filter",
    )(
        pltpu.with_memory_space_constraint(widths, pltpu.HBM),
        pltpu.with_memory_space_constraint(dispersed, pltpu.HBM),
    )
    return pl.pallas_call(
        hand_out,
        out_shape=(
            jax.ShapeDtypeStruct(snr.shape, BF16),
            jax.ShapeDtypeStruct(peaks.shape, F32),
        ),
        in_specs=[pl.BlockSpec(memory_space=pltpu.VMEM)] * 2,
        out_specs=(pl.BlockSpec(memory_space=pltpu.HBM), pl.BlockSpec(memory_space=pltpu.HBM)),
        scratch_shapes=[sems((nbox + 1,))],
        compiler_params=pltpu.CompilerParams(vmem_limit_bytes=1024 * 1024),
        name="hand_out",
    )(snr, peaks)


def solution(mesh):
    return jax.shard_map(
        functools.partial(body, mesh.shape["tm"], mesh.shape["dm"]),
        mesh=mesh,
        in_specs=(P("dm", "tm"), P()),
        out_specs=(P(None, "dm", "tm"), P(None, "dm")),
        check_vma=False,
    )
```

```python
import functools

import jax
import jax.numpy as jnp
from jax import lax
from jax.experimental import pallas as pl
from jax.experimental.pallas import tpu as pltpu
from jax.sharding import PartitionSpec as P

HALF = 128
BLK = 2 * HALF
LANES = 128
ROWS_STEP = 64
PIECES = 3
EPS = 1e-06
MESH = pl.DeviceIdType.MESH
F32 = jnp.float32
BF16 = jnp.bfloat16


def pieces_of(value):
    out = []
    for _ in range(PIECES):
        term = value.astype(BF16)
        out.append(term)
        value = value - term.astype(F32)
    return out


def put_pieces(ref, start, value, span=slice(None)):
    for p, term in enumerate(pieces_of(value)):
        ref[p, span, start : start + value.shape[1]] = term


def window_dot(ref, start, reach, band, span=slice(None)):
    total = None
    for p in range(PIECES):
        part = jnp.dot(ref[p, span, start : start + reach], band, preferred_element_type=F32)
        total = part if total is None else total + part
    return total


def kernel(
    n_tm, n_dm, widths_hbm, x_ref, snr_ref, peaks_ref,
    widths_ref, ahead, squares, xe, xs, fms, det, ds, boxes, band, box_band, power, colsum, top, best,
    width_sem, load_sem, halo_send, halo_recv, power_send, power_recv, col_send, col_recv, top_send, top_recv,
):
    rows, length = x_ref.shape
    nbox = widths_hbm.shape[0]
    blocks = length // BLK
    total_len = n_tm * length
    me = lax.axis_index("tm")
    mine = lax.axis_index("dm")
    offset = me * length
    has_left, has_right = me > 0, me < n_tm - 1
    edge = BLK + length

    def load(k, start, size):
        return pltpu.make_async_copy(
            x_ref.at[:, pl.ds(start, size)], xe.at[:, pl.ds(BLK + start, size)], load_sem.at[k]
        )

    loads = [load(0, 0, BLK), load(1, length - BLK, BLK), load(2, BLK, length - 2 * BLK)]
    width_load = pltpu.make_async_copy(widths_hbm, widths_ref, width_sem)
    width_load.start()
    for one in loads:
        one.start()

    barrier = pltpu.get_barrier_semaphore()
    for d in range(1, n_tm):
        pl.semaphore_signal(barrier, inc=1, device_id={"tm": lax.rem(me + d, n_tm)}, device_id_type=MESH)
    for d in range(1, n_dm):
        pl.semaphore_signal(barrier, inc=1, device_id={"dm": lax.rem(mine + d, n_dm)}, device_id_type=MESH)

    rows_i = lax.broadcasted_iota(jnp.int32, (2 * BLK, BLK), 0)
    cols_i = lax.broadcasted_iota(jnp.int32, (2 * BLK, BLK), 1)
    band[...] = jnp.where((rows_i >= cols_i) & (rows_i <= cols_i + BLK), 1.0, 0.0).astype(BF16)
    width_load.wait()
    rows_b = lax.broadcasted_iota(jnp.int32, (BLK + HALF, BLK), 0)
    cols_b = lax.broadcasted_iota(jnp.int32, (BLK + HALF, BLK), 1)
    lag = rows_b - cols_b
    for i in range(nbox):
        hit = (lag >= 0) & (lag < widths_ref[i])
        box_band[:, i * BLK : (i + 1) * BLK] = jnp.where(hit, 1.0, 0.0).astype(BF16)

    pl.semaphore_wait(barrier, n_tm - 1 + n_dm - 1)

    right = {"tm": lax.rem(me + 1, n_tm)}
    left = {"tm": lax.rem(me + n_tm - 1, n_tm)}

    def move(src, dst, k, target):
        return pltpu.make_async_remote_copy(
            src_ref=src, dst_ref=dst, send_sem=halo_send.at[k], recv_sem=halo_recv.at[k],
            device_id=target, device_id_type=MESH,
        )

    half = rows // 2
    spans = [slice(0, half), slice(half, rows)]

    def right_halo(h):
        span = pl.ds(h * half, half)
        return move(xe.at[span, pl.ds(length, BLK)], xe.at[span, pl.ds(0, BLK)], 2 * h, right)

    def left_halo(h):
        span = pl.ds(h * half, half)
        return move(xe.at[span, pl.ds(BLK, BLK)], xe.at[span, pl.ds(edge, BLK)], 2 * h + 1, left)

    to_right = [right_halo(0), right_halo(1)]
    to_left = [left_halo(0), left_halo(1)]
    beyond = move(xe.at[:, pl.ds(2 * BLK, HALF)], xe.at[:, pl.ds(edge + BLK, HALF)], 4, left)

    loads[1].wait()

    @pl.when(has_right)
    def _():
        for one in to_right:
            one.start()

    loads[0].wait()

    @pl.when(has_left)
    def _():
        for one in to_left:
            one.start()

    @pl.when(jnp.logical_not(has_left))
    def _():
        xe[:, 0:BLK] = jnp.zeros((rows, BLK), F32)

    @pl.when(jnp.logical_not(has_right))
    def _():
        xe[:, edge : edge + BLK + HALF] = jnp.zeros((rows, BLK + HALF), F32)

    loads[2].wait()

    @pl.when(has_left)
    def _():
        beyond.start()

    def inverse_counts(first, size):
        pos = offset + first + lax.broadcasted_iota(jnp.int32, (1, size), 1)
        counts = jnp.minimum(pos + HALF, total_len - 1) - jnp.maximum(pos - HALF, 0) + 1
        inside = (pos >= 0) & (pos < total_len)
        return jnp.where(inside, 1.0 / counts.astype(F32), 0.0)

    def put_mean(start, sums, span=slice(None)):
        put_pieces(fms, start, sums * inverse_counts(start - HALF, sums.shape[1]), span)

    def put_detrended(start, sums, span=slice(None)):
        size = sums.shape[1]
        value = xe[span, BLK + start : BLK + start + size] - sums * inverse_counts(start, size)
        det[span, start : start + size] = value
        put_pieces(ds, start, value, span)

    def square_sum(first, last):
        total = None
        for c in range(first, last, LANES):
            part = det[:, c : c + LANES]
            total = part * part if total is None else total + part * part
        return total

    def full(ref, start):
        return window_dot(ref, start, 2 * BLK, band[...])

    def upper(ref, start, span=slice(None)):
        return window_dot(ref, start, BLK, band[0:BLK, :], span)

    def lower(ref, start, span=slice(None)):
        return window_dot(ref, start, BLK, band[BLK:, :], span)

    last = length - BLK
    for j in range(1, blocks + 1):
        put_pieces(xs, j * BLK, xe[:, j * BLK : (j + 1) * BLK])
    for j in range(1, blocks):
        put_mean(j * BLK, full(xs, j * BLK))
    for j in range(1, blocks - 1):
        put_detrended(j * BLK, full(fms, j * BLK))
    ahead[0] = lower(xs, BLK)
    ahead[1] = upper(xs, length)
    ahead[2] = lower(fms, BLK)
    ahead[3] = upper(fms, last)
    squares[...] = square_sum(BLK, last)

    def left_edge(span):
        put_pieces(xs, 0, xe[span, 0:BLK], span)
        put_mean(0, ahead[0, span] + upper(xs, 0, span), span)
        put_detrended(0, ahead[2, span] + upper(fms, 0, span), span)

    def right_edge(span):
        put_pieces(xs, edge, xe[span, edge : edge + BLK], span)
        put_mean(length, ahead[1, span] + lower(xs, edge, span), span)
        put_detrended(last, ahead[3, span] + lower(fms, length, span), span)

    for h, span in enumerate(spans):
        @pl.when(has_left)
        def _(one=to_right[h]):
            one.wait_recv()

        left_edge(span)

        @pl.when(has_right)
        def _(one=to_left[h]):
            one.wait_recv()

        right_edge(span)

    squares[...] += square_sum(0, BLK)

    def exchange(slots, send, recv, axis, size, index):
        copies = []
        for d in range(1, size):
            copies.append(
                pltpu.make_async_remote_copy(
                    src_ref=slots.at[0], dst_ref=slots.at[d], send_sem=send.at[d], recv_sem=recv.at[d],
                    device_id={axis: lax.rem(index + d, size)}, device_id_type=MESH,
                )
            )
        for one in copies:
            one.start()
        return copies

    all_squares = squares[...] + square_sum(last, length)
    power[0] = jnp.sum(jnp.transpose(all_squares), axis=0, keepdims=True)
    power_copies = exchange(power, power_send, power_recv, "tm", n_tm, me)

    def boxcar(j):
        sums = window_dot(ds, j * BLK, BLK + HALF, box_band[...])
        for i in range(nbox):
            boxes[i, :, j * BLK : (j + 1) * BLK] = sums[:, i * BLK : (i + 1) * BLK]

    early = blocks // 2
    for j in range(early):
        boxcar(j)

    @pl.when(has_right)
    def _():
        beyond.wait_recv()

    short = band[0 : BLK + HALF, 0:HALF]
    put_pieces(xs, edge + BLK, xe[:, edge + BLK : edge + BLK + HALF])
    put_mean(edge, window_dot(xs, edge, BLK + HALF, short))
    put_detrended(length, window_dot(fms, length, BLK + HALF, short))

    for one in power_copies:
        one.wait_recv()
    power_sum = power[0]
    for d in range(1, n_tm):
        power_sum = power_sum + power[d]
    scale = 1.0 / jnp.sqrt(power_sum / total_len + EPS)
    scale_rows = jnp.transpose(jnp.broadcast_to(scale, (LANES, rows)))
    for c in range(length // LANES + 1):
        part = det[:, c * LANES : (c + 1) * LANES] * scale_rows
        colsum[0, :, c * LANES : (c + 1) * LANES] = jnp.sum(part, axis=0, keepdims=True)
    col_copies = exchange(colsum, col_send, col_recv, "dm", n_dm, mine)

    for j in range(early, blocks):
        boxcar(j)

    for one in col_copies:
        one.wait_recv()
    common = colsum[0]
    for d in range(1, n_dm):
        common = common + colsum[d]
    common = common / (rows * n_dm)
    lines = [common[:, j * BLK : (j + 1) * BLK + HALF] for j in range(blocks)]
    lines = lines + [jnp.zeros((-blocks % 8, BLK + HALF), F32)] if blocks % 8 else lines
    stacked = jnp.concatenate(lines, axis=0)
    height = stacked.shape[0]
    terms = jnp.concatenate([term.astype(F32) for term in pieces_of(stacked)], axis=0).astype(BF16)
    parts = jnp.dot(terms, box_band[...], preferred_element_type=F32)
    common_boxes = parts[0:height]
    for p in range(1, PIECES):
        common_boxes = common_boxes + parts[p * height : (p + 1) * height]

    def each_series(use):
        for i in range(nbox):
            width = jnp.full((1, LANES), widths_ref[i], jnp.int32).astype(F32)
            inverse = 1.0 / jnp.sqrt(width)
            shifts = []
            for c in range(length // LANES):
                j, part = divmod(c * LANES, BLK)
                first = i * BLK + part
                shifts.append(common_boxes[j : j + 1, first : first + LANES] * inverse)
            for r in range(rows // ROWS_STEP):
                span = slice(r * ROWS_STEP, (r + 1) * ROWS_STEP)
                factor = scale_rows[span] * inverse
                use(i, span, [
                    boxes[i, span, c * LANES : (c + 1) * LANES] * factor - shifts[c]
                    for c in range(length // LANES)
                ])

    def take_peak(i, span, parts):
        best[i, span, :] = functools.reduce(jnp.maximum, parts)

    def take_snr(i, span, parts):
        for c, series in enumerate(parts):
            snr_ref[i, span, c * LANES : (c + 1) * LANES] = series.astype(BF16)

    each_series(take_peak)
    for i in range(nbox):
        top[0, i : i + 1, :] = jnp.max(jnp.transpose(best[i]), axis=0, keepdims=True)

    top_copies = exchange(top, top_send, top_recv, "tm", n_tm, me)
    each_series(take_snr)
    for one in top_copies:
        one.wait_recv()
    peaks = top[0]
    for d in range(1, n_tm):
        peaks = jnp.maximum(peaks, top[d])
    peaks_ref[...] = peaks

    for one in power_copies + col_copies + top_copies:
        one.wait_send()

    @pl.when(has_right)
    def _():
        for one in to_right:
            one.wait_send()

    @pl.when(has_left)
    def _():
        for one in to_left:
            one.wait_send()
        beyond.wait_send()


def hand_out(snr_ref, peaks_ref, snr_out, peaks_out, sem):
    nbox = snr_ref.shape[0]
    copies = [pltpu.make_async_copy(snr_ref.at[i], snr_out.at[i], sem.at[i]) for i in range(nbox)]
    copies.append(pltpu.make_async_copy(peaks_ref, peaks_out, sem.at[nbox]))
    for one in copies:
        one.start()
    for one in copies:
        one.wait()


def body(n_tm, n_dm, dispersed, widths):
    rows, length = dispersed.shape
    nbox = widths.shape[0]
    sems = pltpu.SemaphoreType.DMA
    snr, peaks = pl.pallas_call(
        functools.partial(kernel, n_tm, n_dm),
        out_shape=(
            jax.ShapeDtypeStruct((nbox, rows, length), BF16),
            jax.ShapeDtypeStruct((nbox, rows), F32),
        ),
        in_specs=[pl.BlockSpec(memory_space=pltpu.HBM)] * 2,
        out_specs=(pl.BlockSpec(memory_space=pltpu.VMEM), pl.BlockSpec(memory_space=pltpu.VMEM)),
        scratch_shapes=[
            pltpu.SMEM((nbox,), jnp.int32),
            pltpu.VMEM((4, rows, BLK), F32),
            pltpu.VMEM((rows, LANES), F32),
            pltpu.VMEM((rows, length + 2 * BLK + HALF), F32),
            pltpu.VMEM((PIECES, rows, length + 2 * BLK + HALF), BF16),
            pltpu.VMEM((PIECES, rows, length + BLK + HALF), BF16),
            pltpu.VMEM((rows, length + HALF), F32),
            pltpu.VMEM((PIECES, rows, length + HALF), BF16),
            pltpu.VMEM((nbox, rows, length), F32),
            pltpu.VMEM((2 * BLK, BLK), BF16),
            pltpu.VMEM((BLK + HALF, nbox * BLK), BF16),
            pltpu.VMEM((n_tm, 1, rows), F32),
            pltpu.VMEM((n_dm, 1, length + HALF), F32),
            pltpu.VMEM((n_tm, nbox, rows), F32),
            pltpu.VMEM((nbox, rows, LANES), F32),
            sems, sems((3,)), sems((5,)), sems((5,)),
            sems((n_tm,)), sems((n_tm,)),
            sems((n_dm,)), sems((n_dm,)),
            sems((n_tm,)), sems((n_tm,)),
        ],
        compiler_params=pltpu.CompilerParams(
            collective_id=0, has_side_effects=True, vmem_limit_bytes=40 * 1024 * 1024
        ),
        name="detrend_filter",
    )(
        pltpu.with_memory_space_constraint(widths, pltpu.HBM),
        pltpu.with_memory_space_constraint(dispersed, pltpu.HBM),
    )
    return pl.pallas_call(
        hand_out,
        out_shape=(
            jax.ShapeDtypeStruct(snr.shape, BF16),
            jax.ShapeDtypeStruct(peaks.shape, F32),
        ),
        in_specs=[pl.BlockSpec(memory_space=pltpu.VMEM)] * 2,
        out_specs=(pl.BlockSpec(memory_space=pltpu.HBM), pl.BlockSpec(memory_space=pltpu.HBM)),
        scratch_shapes=[sems((nbox + 1,))],
        compiler_params=pltpu.CompilerParams(vmem_limit_bytes=1024 * 1024),
        name="hand_out",
    )(snr, peaks)


def solution(mesh):
    return jax.shard_map(
        functools.partial(body, mesh.shape["tm"], mesh.shape["dm"]),
        mesh=mesh,
        in_specs=(P("dm", "tm"), P()),
        out_specs=(P(None, "dm", "tm"), P(None, "dm")),
        check_vma=False,
    )
```
